32 devices in a mesh: pts: 16 (over z, x, core), grp: 2 (over y).
Axes of the slice: x: 2, y: 2, z: 4, core: 2. Of those that a mesh axis runs over, the one named last changes fastest.
Arguments:
- cam_jac: float32 [2, 9, 219136], P(None, None, ('pts', 'grp')), may hold values from -6 to 6
- pt_jac: float32 [2, 3, 219136], P(None, None, ('pts', 'grp')), may hold values from -6 to 6
- cam_slot: int32 [219136], P(('pts', 'grp')), may hold values from 0 to 127
- obs_point: int32 [219136], P(('pts', 'grp')), may hold values from 0 to 2047
- cam_inverse: float32 [9, 9, 13696], replicated, may hold values from -1 to 1, as said below
- pt_inverse: float32 [3, 3, 65536], P(None, None, ('pts', 'grp')), may hold values from -1 to 1, as said below
- cam_rhs: float32 [9, 13696], replicated, may hold values from -48 to 48
- pt_rhs: float32 [3, 65536], P(None, ('pts', 'grp')), may hold values from -240 to 240
Outputs:
- camera_step: float32 [9, 13696], replicated
- point_step: float32 [3, 65536], P(None, ('pts', 'grp'))
- resid_ratio: float32 [], replicated
The draws below stay inside these ranges and needn't reach their ends.
Inputs may be any that keep to these rules, and one draw needn't show every extreme that they name: The observations of each device come in 107 runs of 64; run b holds observations of cameras b * 128 to (b + 1) * 128 - 1, and cam_slot is the camera's offset in that run's block. The point of observation o is (o // 6848) * 2048 + obs_point[o]. `cam_inverse`: each camera's 9 x 9 block is symmetric positive definite. `pt_inverse`: each point's 3 x 3 block is symmetric positive definite.
All inputs are finite; a program needn't handle non-finite values.
Results may differ from the reference program's by a relative error of at most 0.00014.
Values sent between devices are 32-bit elements; how exact they have to be, the bound alone decides.
A program may use at most 128 MiB of HBM per device.

```python
import math
import jax
import jax.numpy as jnp
from jax import lax

CAM_BLK = 128
CAMS = 13696
SLOTS = 64
PTS_DEV = 2048
TERMS = 3
OBS_DEV = 6848
OBS = 219136
PTS = 65536
CAM_OBS = 16


def spd_blocks(key, order, count, low, high, coupling):
    key_scale, key_offdiag = jax.random.split(key)
    scales = jnp.exp(jax.random.uniform(key_scale, (order, count), jnp.float32, math.log(low), math.log(high)))
    offdiag = jax.random.uniform(key_offdiag, (order, order, count), jnp.float32, -coupling, coupling)
    offdiag = 0.5 * (offdiag + jnp.transpose(offdiag, (1, 0, 2)))
    identity = jnp.eye(order, dtype=jnp.float32)[:, :, None]
    coupled = identity + offdiag * (1.0 - identity)
    roots = jnp.sqrt(scales)
    return roots[:, None, :] * coupled * roots[None, :, :]


def draw_cam_inverse(key, part):
    return spd_blocks(key, 9, CAMS, 0.4 / CAM_OBS, 1.6 / CAM_OBS, 0.11)


def draw_pt_inverse(key, part):
    return spd_blocks(key, 3, PTS, 0.03, 0.3, 0.4)


def draw_pt_rhs(key, part):
    ramp = jnp.arange(PTS, dtype=jnp.float32) / PTS
    noise = jnp.clip(jax.random.normal(key, (3, PTS), jnp.float32), -5.0, 5.0)
    return 16.0 * noise * (1.0 + 2.0 * ramp)[None, :]


def place_ends(drawn, stream_key, least, high):
    dims = drawn.shape
    spot = [jax.random.randint(jax.random.fold_in(stream_key, axis), (), 0, dims[axis]) for axis in range(len(dims))]
    drawn = drawn.at[tuple(spot)].set(least)
    longest = dims.index(max(dims))
    spot[longest] = (spot[longest] + 1) % dims[longest]
    return drawn.at[tuple(spot)].set(high)


def block_scale(stream_key, extent, cuts, low, top_value):
    loudness, own = 1.0, jax.random.fold_in(stream_key, 6)
    for dim, shards_of in cuts:
        steps = jnp.exp(jax.random.uniform(jax.random.fold_in(own, dim), (shards_of,), jnp.float32, low / len(cuts), top_value / len(cuts)))
        loudness = loudness * jnp.repeat(steps, extent[dim] // shards_of).reshape([-1 if axis == dim else 1 for axis in range(len(extent))])
    return loudness


def scatter_about(key, extent, width, reach, cuts=(), kind=jnp.bfloat16):
    array = jax.random.normal(key, extent, jnp.float32) * width
    if len(cuts) > 0:
        array = block_scale(key, extent, cuts, -0.22, 0.18) * array
    return jnp.clip(array, min=-reach, max=reach).astype(kind)


def setup_inputs(seed: int = 0) -> dict:
    seeds = jax.random.split(jax.random.key(seed), 9)
    return {
        "cam_jac": scatter_about(seeds[0], (2, 9, OBS), 1.0, 6.0, ((2, 32),), jnp.float32),
        "pt_jac": scatter_about(seeds[1], (2, 3, OBS), 1.0, 6.0, ((2, 32),), jnp.float32),
        "cam_slot": place_ends(jax.random.randint(seeds[2], (OBS,), 0, CAM_BLK), jax.random.fold_in(seeds[2], 1), 0, CAM_BLK - 1).astype(jnp.int32),
        "obs_point": place_ends(jax.random.randint(seeds[3], (OBS,), 0, PTS_DEV), jax.random.fold_in(seeds[3], 1), 0, PTS_DEV - 1).astype(jnp.int32),
        "cam_inverse": draw_cam_inverse(jax.random.fold_in(seeds[8], 71), 0),
        "pt_inverse": draw_pt_inverse(jax.random.fold_in(seeds[8], 71), 0),
        "cam_rhs": scatter_about(seeds[6], (9, CAMS), (0.5 * CAM_OBS), 48.0, (), jnp.float32),
        "pt_rhs": draw_pt_rhs(jax.random.fold_in(seeds[8], 71), 0),
    }


def reference(cam_jac, pt_jac, cam_slot, obs_point, cam_inverse, pt_inverse, cam_rhs, pt_rhs):
    total = cam_slot.shape[0]
    cameras = cam_rhs.shape[1]
    points = pt_rhs.shape[1]
    positions = jnp.arange(total, dtype=jnp.int32)
    cam_index = positions % OBS_DEV // SLOTS * CAM_BLK + cam_slot
    pt_index = positions // OBS_DEV * PTS_DEV + obs_point

    def to_points(camera_vec):
        at_obs = camera_vec[:, cam_index]
        projected = lax.optimization_barrier(jnp.sum(cam_jac * at_obs[None], axis=1))
        lifted = lax.optimization_barrier(jnp.sum(pt_jac * projected[:, None], axis=0))
        return jnp.zeros((3, points), jnp.float32).at[:, pt_index].add(lifted)

    def to_cameras(point_vec):
        at_obs = point_vec[:, pt_index]
        projected = lax.optimization_barrier(jnp.sum(pt_jac * at_obs[None], axis=1))
        pulled = lax.optimization_barrier(jnp.sum(cam_jac * projected[:, None], axis=0))
        return jnp.zeros((9, cameras), jnp.float32).at[:, cam_index].add(pulled)

    def point_solve(point_vec):
        return lax.optimization_barrier(jnp.sum(pt_inverse * point_vec[None], axis=1))

    def camera_solve(camera_vec):
        return lax.optimization_barrier(jnp.sum(cam_inverse * camera_vec[None], axis=1))
    reduced = cam_rhs - to_cameras(point_solve(pt_rhs))
    series_term = camera_solve(reduced)
    camera_step = series_term
    for series_index in range(TERMS):
        series_term = camera_solve(to_cameras(point_solve(to_points(series_term))))
        camera_step = camera_step + series_term
    point_resid = pt_rhs - to_points(camera_step)
    point_step = point_solve(point_resid)
    resid_ratio = jnp.sqrt(jnp.sum(point_resid * point_resid) / jnp.sum(pt_rhs * pt_rhs))
    return (camera_step, point_step, resid_ratio)
```

```python
import functools

import jax
import jax.numpy as jnp
from jax import lax
from jax.experimental import pallas as pl
from jax.experimental.pallas import tpu as pltpu
from jax.sharding import PartitionSpec as P

CAM_BLK = 128
TERMS = 3
MESH = pl.DeviceIdType.MESH
VMEM = pl.BlockSpec(memory_space=pltpu.VMEM)
F32 = jnp.float32
BF16 = jnp.bfloat16


def halves(v):
    top = v.astype(BF16)
    return top, (v - top.astype(F32)).astype(BF16)


def prepare(obs, live, per, msg, cj_in, pj_in, slot_in, point_in, cjm, pj, slot, point):
    slot[...] = jnp.zeros_like(slot)
    point[...] = jnp.zeros_like(point)
    for r in range(live):
        span = min(128, obs - r * 128)
        cols = slice(r * 128, r * 128 + span)
        slot[r : r + 1, 0:span] = slot_in[cols].reshape(1, span)
        point[r : r + 1, 0:span] = point_in[cols].reshape(1, span)
        base = (r // per) * msg + (r % per) * 18
        for j in range(9):
            cjm[base + 2 * j : base + 2 * j + 2, 0:span] = cj_in[j, :, cols]
        for i in range(3):
            pj[(i * 64 + r) * 2 : (i * 64 + r) * 2 + 2, 0:span] = pj_in[i, :, cols]
        if span < 128:
            cjm[base : base + 18, span:128] = jnp.zeros((18, 128 - span), F32)
            for i in range(3):
                pj[(i * 64 + r) * 2 : (i * 64 + r) * 2 + 2, span:128] = jnp.zeros((2, 128 - span), F32)
    for i in range(3):
        pj[(i * 64 + live) * 2 : (i * 64 + 64) * 2, :] = jnp.zeros(((64 - live) * 2, 128), F32)


def prepare_points(live, pinv_in, prhs_in, point, pinv, prhs, right):
    for s in range(16):
        cols = slice(s * 128, s * 128 + 128)
        prhs[pl.ds(s, 3, stride=16), :] = prhs_in[:, cols]
        for i in range(3):
            pinv[pl.ds(48 * i + s, 3, stride=16), :] = pinv_in[i, :, cols]
    low = lax.broadcasted_iota(jnp.int32, (128, 128), 0)
    for r in range(live):
        cols = slice(r * 128, (r + 1) * 128)
        right[:, cols] = jnp.where(low == (point[r : r + 1, :] & 127), 1.0, 0.0).astype(BF16)


def point_solve(pinv, y):
    out = []
    for i in range(3):
        row = 48 * i
        out.append(
            pinv[row : row + 16] * y[0:16] + pinv[row + 16 : row + 32] * y[16:32] + pinv[row + 32 : row + 48] * y[32:48]
        )
    return jnp.concatenate(out, axis=0)


def from_points(groups, z, pj, point, s_out):
    for g in range(groups):
        where = point[8 * g : 8 * g + 8, :]
        low, high = where & 127, where >> 7
        got = [jnp.zeros((8, 128), F32)] * 3
        for s in range(16):
            hit = high == s
            for i in range(3):
                table = jnp.broadcast_to(z[16 * i + s : 16 * i + s + 1, :], (8, 128))
                cand = jnp.take_along_axis(table, low, axis=1, mode="promise_in_bounds")
                got[i] = jnp.where(hit, cand, got[i])
        for a in range(2):
            part = None
            for i in range(3):
                term = pj[pl.ds((i * 64 + 8 * g) * 2 + a, 8, stride=2), :] * got[i]
                part = term if part is None else part + term
            s_out[pl.ds(16 * g + a, 8, stride=2), :] = part


def onto_points(live, groups, r_in, pj, point, quant, left, right):
    for g in range(groups):
        proj = [r_in[pl.ds(16 * g + a, 8, stride=2), :] for a in range(2)]
        for i in range(3):
            quant[64 * i + 8 * g : 64 * i + 8 * g + 8, :] = (
                pj[pl.ds((i * 64 + 8 * g) * 2, 8, stride=2), :] * proj[0]
                + pj[pl.ds((i * 64 + 8 * g) * 2 + 1, 8, stride=2), :] * proj[1]
            )
    high = lax.broadcasted_iota(jnp.int32, (16, 128), 0)
    for r in range(live):
        cols = slice(r * 128, (r + 1) * 128)
        hit = high == (point[r : r + 1, :] >> 7)
        for i in range(3):
            v = jnp.where(hit, quant[64 * i + r : 64 * i + r + 1, :], 0.0)
            top, rest = halves(v)
            left[i * 16 : i * 16 + 16, cols] = top
            left[48 + i * 16 : 64 + i * 16, cols] = rest
    both = lax.dot_general(left[...], right[...], (((1,), (1,)), ((), ())), preferred_element_type=F32)
    return both[0:48] + both[48:96]


def build_hot(n, per, slots, hot):
    low = lax.broadcasted_iota(jnp.int32, (128, 128), 0)
    for src in range(n):
        for p in range(per):
            row = src * per + p
            hot[p, :, src * 128 : src * 128 + 128] = jnp.where(low == slots[row : row + 1, :], 1.0, 0.0).astype(BF16)


def gather_blocks(n, per, msg, s_in, cjo, hot, pull, lhs):
    width = 2 * per
    for g in range(n // 8):
        for p in range(per):
            s = [s_in[pl.ds(8 * g * width + 2 * p + a, 8, stride=width), :] for a in range(2)]
            for j in range(9):
                at = 8 * g * msg + p * 18 + 2 * j
                pull[pl.ds((8 * g * per + p) * 16 + j, 8, stride=16 * per), :] = (
                    cjo[pl.ds(at, 8, stride=msg), :] * s[0] + cjo[pl.ds(at + 1, 8, stride=msg), :] * s[1]
                )
    lane_low = lax.broadcasted_iota(jnp.int32, (16, 128), 1) < 64
    sums = []
    for p in range(per):
        for src in range(n):
            cols = slice(src * 128, src * 128 + 128)
            base = (src * per + p) * 16
            v = pull[base : base + 16, :]
            e_top, e_rest = halves(jnp.where(lane_low, v, 0.0))
            o_top, o_rest = halves(jnp.where(lane_low, 0.0, v))
            for k, piece in enumerate((e_top, e_rest, o_top, o_rest)):
                lhs[p, 16 * k : 16 * k + 16, cols] = piece
        d = lax.dot_general(lhs[p], hot[p], (((1,), (1,)), ((), ())), preferred_element_type=F32)
        sums.append((d[0:16] + d[16:32])[0:9])
        sums.append((d[32:48] + d[48:64])[0:9])
    return sums


def spread_blocks(n, per, msg, xs, slots, cjo, r_out):
    width = 2 * per
    lane_low = lax.broadcasted_iota(jnp.int32, (8, 128), 1) < 64
    for g in range(n // 8):
        for p in range(per):
            index = slots[pl.ds(8 * g * per + p, 8, stride=per), :]
            proj = [None, None]
            for j in range(9):
                row = 32 * p + j
                even = jnp.broadcast_to(xs[row : row + 1, :], (8, 128))
                odd = jnp.broadcast_to(xs[row + 16 : row + 17, :], (8, 128))
                even = jnp.take_along_axis(even, index, axis=1, mode="promise_in_bounds")
                odd = jnp.take_along_axis(odd, index, axis=1, mode="promise_in_bounds")
                got = jnp.where(lane_low, even, odd)
                for a in range(2):
                    part = cjo[pl.ds(8 * g * msg + p * 18 + 2 * j + a, 8, stride=msg), :] * got
                    proj[a] = part if proj[a] is None else proj[a] + part
            for a in range(2):
                r_out[pl.ds(8 * g * width + 2 * p + a, 8, stride=width), :] = proj[a]


def body(
    n, grp_size, blocks, per, owners, msg, live, groups, obs,
    cj_in, pj_in, slot_in, point_in, pinv_in, prhs_in, cinv, crhs,
    cam_out, pt_out, ratio_out,
    cjm, pj, slot, point, pinv, prhs, right, left, quant, zs, s_out, r_in,
    cjo, sloto, hot, pull, lhs, s_in, r_out, xs, inv, rhs, kept, final, fin, mine, sums,
    load, slot_s, slot_r, jac_s, jac_r, s_s, s_r, r_s, r_r, f_s, f_r, q_s, q_r,
):
    me = lax.axis_index("pts") * grp_size + lax.axis_index("grp")
    width = 2 * per
    is_owner = me < owners

    def at(other):
        return (other // grp_size, lax.rem(other, grp_size))

    def others(step):
        def run(k, carry):
            step(jnp.bitwise_xor(me, n - k))
            return carry

        lax.fori_loop(1, n, run, 0)

    barrier = pltpu.get_barrier_semaphore()
    others(lambda d: pl.semaphore_signal(barrier, inc=1, device_id=at(d), device_id_type=MESH))

    def loads(q):
        cols = pl.ds(pl.multiple_of((me * width + q) * 128, 128), 128)
        return (
            pltpu.make_async_copy(cinv.at[:, :, cols], inv.at[q], load.at[2 * q]),
            pltpu.make_async_copy(crhs.at[:, cols], rhs.at[q], load.at[2 * q + 1]),
        )

    for q in range(width):
        @pl.when(me * width + q < blocks)
        def _():
            for copy in loads(q):
                copy.start()

        @pl.when(me * width + q >= blocks)
        def _():
            inv[q] = jnp.zeros((9, 9, 128), F32)
            rhs[q] = jnp.zeros((9, 128), F32)

    prepare(obs, live, per, msg, cj_in, pj_in, slot_in, point_in, cjm, pj, slot, point)

    def rows(ref, index, count):
        return ref.at[pl.ds(index * count, count)]

    def send(src, src_at, dst, dst_at, count, send_sem, recv_sem, device):
        return pltpu.make_async_remote_copy(
            src_ref=rows(src, src_at, count), dst_ref=rows(dst, dst_at, count),
            send_sem=send_sem, recv_sem=recv_sem, device_id=at(device), device_id_type=MESH,
        )

    def wait_sent(src, count, send_sem, recv_sem):
        part = src.at[pl.ds(0, count)]
        pltpu.make_async_remote_copy(
            src_ref=part, dst_ref=part, send_sem=send_sem, recv_sem=recv_sem, device_id=at(me), device_id_type=MESH
        ).wait_send()

    def wait_got(dst, count, send_sem, recv_sem):
        part = dst.at[pl.ds(0, count)]
        pltpu.make_async_remote_copy(
            src_ref=part, dst_ref=part, send_sem=send_sem, recv_sem=recv_sem, device_id=at(me), device_id_type=MESH
        ).wait_recv()

    def keep(src, src_at, dst, dst_at, count):
        for k in range(count):
            dst[pl.ds(dst_at * count + k, 1), :] = src[pl.ds(src_at * count + k, 1), :]

    def to_owners(make):
        others(lambda d: pl.when(d < owners)(lambda: make(d).start()))

    def by_role(step):
        pl.when(is_owner)(lambda: step(owners - 1))
        pl.when(jnp.logical_not(is_owner))(lambda: step(owners))

    pl.semaphore_wait(barrier, n - 1)
    to_owners(lambda d: send(slot, d, sloto, me, per, slot_s, slot_r, d))
    to_owners(lambda d: send(cjm, d, cjo, me, msg, jac_s, jac_r, d))
    prepare_points(live, pinv_in, prhs_in, point, pinv, prhs, right)
    zs[...] = prhs[...]
    kept[...] = jnp.zeros_like(kept)
    pull[...] = jnp.zeros_like(pull)
    final[...] = jnp.zeros_like(final)
    r_in[...] = jnp.zeros_like(r_in)
    for q in range(width):
        @pl.when(me * width + q < blocks)
        def _():
            for copy in loads(q):
                copy.wait()

    @pl.when(is_owner)
    def _():
        keep(slot, me, sloto, me, per)
        keep(cjm, me, cjo, me, msg)
        wait_got(sloto, (n - 1) * per, slot_s, slot_r)
        build_hot(n, per, sloto, hot)

    def term(index, carry):
        zs[...] = point_solve(pinv, zs[...])
        from_points(groups, zs, pj, point, s_out)
        to_owners(lambda d: send(s_out, d, s_in, me, width, s_s, s_r, d))

        @pl.when(is_owner)
        def _():
            keep(s_out, me, s_in, me, width)

            @pl.when(index == 0)
            def _():
                wait_got(cjo, (n - 1) * msg, jac_s, jac_r)

            wait_got(s_in, (n - 1) * width, s_s, s_r)
            sums = gather_blocks(n, per, msg, s_in, cjo, hot, pull, lhs)
            for q in range(width):
                total = jnp.where(index == 0, rhs[q] - sums[q], sums[q])
                piece = None
                for j in range(9):
                    part = inv[q, j] * total[j : j + 1, :]
                    piece = part if piece is None else piece + part
                step = kept[q] + piece
                kept[q] = step
                final[9 * q : 9 * q + 9, :] = step
                xs[16 * q : 16 * q + 9, :] = jnp.where(index == TERMS, step, piece)
            spread_blocks(n, per, msg, xs, sloto, cjo, r_out)
            others(lambda d: send(r_out, d, r_in, me, width, r_s, r_r, d).start())
            keep(r_out, me, r_in, me, width)

        by_role(lambda count: wait_got(r_in, count * width, r_s, r_r))
        zs[...] = onto_points(live, groups, r_in, pj, point, quant, left, right)
        by_role(lambda count: wait_sent(s_out, count * width, s_s, s_r))
        pl.when(is_owner)(lambda: wait_sent(r_out, (n - 1) * width, r_s, r_r))
        return carry

    lax.fori_loop(0, TERMS + 1, term, 0)

    @pl.when(is_owner)
    def _():
        others(lambda d: send(final, 0, fin, me, msg, f_s, f_r, d).start())
        for k in range(msg // 8):
            fin[pl.ds(pl.multiple_of(me * msg + 8 * k, 8), 8), :] = final[8 * k : 8 * k + 8, :]

    rhs_pts = prhs[...]
    resid = rhs_pts - zs[...]
    for row, vals in ((0, resid * resid), (1, rhs_pts * rhs_pts)):
        mine[row : row + 1, :] = jnp.sum(vals, axis=0, keepdims=True)
    others(lambda d: send(mine, 0, sums, me, 2, q_s, q_r, d).start())
    keep(mine, 0, sums, me, 2)
    zs[...] = point_solve(pinv, resid)
    for s in range(16):
        pt_out[:, s * 128 : s * 128 + 128] = zs[pl.ds(s, 3, stride=16), :]
    by_role(lambda count: wait_sent(slot, count * per, slot_s, slot_r))
    by_role(lambda count: wait_sent(cjm, count * msg, jac_s, jac_r))
    wait_got(sums, (n - 1) * 2, q_s, q_r)
    total = sums[0:8, :]
    for k in range(1, n // 4):
        total = total + sums[8 * k : 8 * k + 8, :]
    even = lax.broadcasted_iota(jnp.int32, (8, 128), 0) % 2 == 0
    top = jnp.sum(jnp.where(even, total, 0.0), keepdims=True)
    low = jnp.sum(jnp.where(even, 0.0, total), keepdims=True)
    ratio_out[...] = jnp.sqrt(top / low)
    by_role(lambda count: wait_got(fin, count * msg, f_s, f_r))
    for b in range(blocks):
        base = (b // width) * msg + (b % width) * 9
        cam_out[:, b * 128 : b * 128 + 128] = fin[base : base + 9, :]

    @pl.when(is_owner)
    def _():
        for _ in range(n - 1):
            wait_sent(final, msg, f_s, f_r)

    for _ in range(n - 1):
        wait_sent(mine, 2, q_s, q_r)


def local(pts_size, grp_size, cam_jac, pt_jac, cam_slot, obs_point, cam_inverse, pt_inverse, cam_rhs, pt_rhs):
    n = pts_size * grp_size
    obs = cam_slot.shape[0]
    cameras = cam_rhs.shape[1]
    blocks = cameras // CAM_BLK
    points = pt_rhs.shape[1]
    live = -(-obs // 128)
    per = -(-live // n)
    owners = -(-live // per)
    msg = -(-18 * per // 8) * 8
    groups = -(-live // 8)
    width = 2 * per
    assert obs == blocks * 64 and points == 2048 and n % 8 == 0 and n & (n - 1) == 0 and live <= 56

    def vmem(*shape):
        return pltpu.VMEM(shape, F32)

    dma = pltpu.SemaphoreType.DMA
    anywhere = pl.BlockSpec(memory_space=pl.ANY)
    wide = live * 128
    camera_step, point_step, ratio = pl.pallas_call(
        functools.partial(body, n, grp_size, blocks, per, owners, msg, live, groups, obs),
        out_shape=(
            jax.ShapeDtypeStruct((9, cameras), F32),
            jax.ShapeDtypeStruct((3, points), F32),
            jax.ShapeDtypeStruct((1, 1), F32),
        ),
        in_specs=[VMEM] * 6 + [anywhere] * 2,
        out_specs=(VMEM, VMEM, VMEM),
        scratch_shapes=[
            vmem(owners * msg, 128), vmem(6 * 64, 128), pltpu.VMEM((64, 128), jnp.int32),
            pltpu.VMEM((64, 128), jnp.int32), vmem(9 * 16, 128), vmem(48, 128),
            pltpu.VMEM((128, wide), BF16), pltpu.VMEM((96, wide), BF16),
            vmem(3 * 64, 128), vmem(48, 128), vmem(16 * groups, 128), vmem(16 * groups, 128),
            vmem(n * msg, 128), pltpu.VMEM((n * per, 128), jnp.int32), pltpu.VMEM((per, 128, n * 128), BF16),
            vmem(n * per * 16, 128), pltpu.VMEM((per, 64, n * 128), BF16),
            vmem(n * width, 128), vmem(n * width, 128), vmem(width * 16, 128),
            vmem(width, 9, 9, 128), vmem(width, 9, 128), vmem(width, 9, 128),
            vmem(msg, 128), vmem(owners * msg, 128), vmem(2, 128), vmem(2 * n, 128),
            dma((2 * width,)), dma, dma, dma, dma, dma, dma, dma, dma, dma, dma, dma, dma,
        ],
        compiler_params=pltpu.CompilerParams(collective_id=0, has_side_effects=True),
        name="schur",
    )(
        jnp.transpose(cam_jac, (1, 0, 2)), jnp.transpose(pt_jac, (1, 0, 2)), cam_slot, obs_point,
        pt_inverse, pt_rhs, cam_inverse, cam_rhs,
    )
    return camera_step, point_step, ratio.reshape(())


def solution(mesh):
    placed = (
        P(None, None, ("pts", "grp")),
        P(None, None, ("pts", "grp")),
        P(("pts", "grp")),
        P(("pts", "grp")),
        P(),
        P(None, None, ("pts", "grp")),
        P(),
        P(None, ("pts", "grp")),
    )
    return jax.shard_map(
        functools.partial(local, mesh.shape["pts"], mesh.shape["grp"]),
        mesh=mesh,
        in_specs=placed,
        out_specs=(P(), P(None, ("pts", "grp")), P()),
        check_vma=False,
    )
```
